32 devices in a mesh: grid: 2 (over x), prow: 4 (over y, core), pcol: 4 (over z).
Axes of the slice: x: 2, y: 2, z: 4, core: 2. Of those that a mesh axis runs over, the one named last changes fastest.
Arguments:
- sub_rhs: float32 [2, 3, 64, 3072], P('grid', None, None, 'prow'), may hold values from -6 to 6
- root_rhs: float32 [64, 3072], P(None, 'prow'), may hold values from -6 to 6
- diag_inverse: bfloat16 [3, 3072, 6144], P(None, 'prow', ('grid', 'pcol'))
- root_inverse: bfloat16 [3072, 3072], P('prow', 'grid')
- inner_factor: bfloat16 [3, 6144, 3072], P(None, ('grid', 'pcol'), 'prow'), may hold values from -0.078125 to 0.078125
- inner_mask: int32 [3, 48, 24], P(None, ('grid', 'pcol')), may hold values 0 or 1
- root_factor: bfloat16 [3, 6144, 3072], P(None, ('grid', 'pcol'), 'prow'), may hold values from -0.078125 to 0.078125
- root_mask: int32 [3, 48, 24], P(None, ('grid', 'pcol')), may hold values 0 or 1
Outputs:
- sub_solution: float32 [3, 64, 6144], P(None, None, ('grid', 'pcol'))
- root_solution: float32 [64, 3072], P(None, 'grid')
The draws below stay inside these ranges and needn't reach their ends.
Inputs may be any that keep to these rules, and one draw needn't show every extreme that they name: `inner_mask`: 1 keeps a tile of 128 x 128 entries, 0 makes it zero. `root_mask`: 1 keeps a tile of 128 x 128 entries, 0 makes it zero.
All inputs are finite; a program needn't handle non-finite values. No bound on the sum of `inner_mask` or of `root_mask` on one device may be relied on, other than what follows from the above.
Results may differ from the reference program's by a relative error of at most 0.0065.
Values sent between devices are 32-bit elements; how exact they have to be, the bound alone decides.
A program may use at most 64 MiB of HBM per device.

```python
import jax
import jax.numpy as jnp

NS = 3072
NRHS = 64
LEVELS = 3
TILE = 128
SUBTREES = 2
PAIRS = 3
TB = 24


def spread_of(key, shape):
    return jax.random.normal(key, shape, jnp.float32) * (0.4 / NS ** 0.5)


def draw_diag_inverse(key, part):
    base = jax.random.fold_in(key, 11)
    first, second = jax.random.split(base)
    diagonal = jax.random.uniform(first, (LEVELS, SUBTREES, NS), jnp.float32, 1.0, 2.0)
    spread = spread_of(second, (LEVELS, NS, SUBTREES * NS))
    identity = jnp.eye(NS, dtype=jnp.float32)
    placed = identity[None, :, None, :] * diagonal[:, None, :, :]
    whole = spread + placed.reshape(LEVELS, NS, SUBTREES * NS)
    return whole.astype(jnp.bfloat16)


def draw_root_inverse(key, part):
    base = jax.random.fold_in(key, 23)
    first, second = jax.random.split(base)
    diagonal = jax.random.uniform(first, (NS,), jnp.float32, 1.0, 2.0)
    spread = spread_of(second, (NS, NS))
    whole = spread + diagonal[:, None] * jnp.eye(NS, dtype=jnp.float32)
    return whole.astype(jnp.bfloat16)


def place_ends(entries, stream_key, smallest, top_value):
    place = [jax.random.randint(jax.random.fold_in(stream_key, axis), (), 0, length) for axis, length in enumerate(entries.shape)]
    widest = entries.shape.index(max(entries.shape))
    neighbour = place[:widest] + [(place[widest] + 1) % entries.shape[widest]] + place[widest + 1:]
    return entries.at[tuple(place)].set(smallest).at[tuple(neighbour)].set(top_value)


def levels(stream_key, extent, cuts, low, largest):
    gain = 1.0
    for dim, shards_of in cuts:
        draws = jax.random.uniform(jax.random.fold_in(jax.random.fold_in(stream_key, 6), dim), (shards_of,), jnp.float32, low / len(cuts), largest / len(cuts))
        gain = gain * jnp.repeat(jnp.exp(draws), extent[dim] // shards_of).reshape((-1,) + (1,) * (len(extent) - 1 - dim))
    return gain


def normal_values(stream_key, dims, width, most, pieces=(), kind=jnp.bfloat16):
    array = jax.random.normal(stream_key, dims, jnp.float32) * width
    if len(pieces) > 0:
        array = levels(stream_key, dims, pieces, -0.22, 0.18) * array
    return jnp.clip(array, min=-most, max=most).astype(kind)


def setup_inputs(seed: int = 0) -> dict:
    streams_of = jax.random.split(jax.random.key(seed), 9)
    sub_rhs = normal_values(streams_of[0], (SUBTREES, LEVELS, NRHS, NS), 1.0, 6.0, ((0, 2), (3, 4)), jnp.float32)
    root_rhs = normal_values(streams_of[1], (NRHS, NS), 1.0, 6.0, ((1, 4),), jnp.float32)
    diag_inverse = draw_diag_inverse(jax.random.fold_in(streams_of[8], 71), 0)
    root_inverse = draw_root_inverse(jax.random.fold_in(streams_of[8], 71), 0)
    inner_factor = normal_values(streams_of[4], (PAIRS, SUBTREES * NS, NS), (2 * NS) ** -0.5, 0.078125, ((1, 8), (2, 4)))
    inner_mask = place_ends((jax.random.randint(streams_of[5], (PAIRS, SUBTREES * TB, TB), 0, 4) < 3).astype(jnp.int32), jax.random.fold_in(streams_of[5], 1), 0, 1)
    root_factor = normal_values(streams_of[6], (LEVELS, SUBTREES * NS, NS), (2 * NS) ** -0.5, 0.078125, ((1, 8), (2, 4)))
    root_mask = place_ends((jax.random.randint(streams_of[7], (LEVELS, SUBTREES * TB, TB), 0, 4) < 3).astype(jnp.int32), jax.random.fold_in(streams_of[7], 1), 0, 1)
    return dict(sub_rhs=sub_rhs, root_rhs=root_rhs, diag_inverse=diag_inverse, root_inverse=root_inverse, inner_factor=inner_factor, inner_mask=inner_mask, root_factor=root_factor, root_mask=root_mask)


def expand(mask):
    wide = jnp.repeat(jnp.repeat(mask, TILE, axis=0), TILE, axis=1)
    return wide.astype(jnp.bfloat16)


def reference(sub_rhs, root_rhs, diag_inverse, root_inverse, inner_factor, inner_mask, root_factor, root_mask):
    root_update = jnp.zeros((NRHS, NS), jnp.float32)
    results = []
    for tree in range(SUBTREES):
        first_row = tree * NS
        first_tile = tree * TB
        kept = []
        levels_out = []
        pair = 0
        for level in range(LEVELS):
            update = jnp.zeros((NRHS, NS), jnp.float32)
            for source in range(level):
                factor = inner_factor[pair, first_row:first_row + NS]
                block = factor * expand(inner_mask[pair, first_tile:first_tile + TB])
                update = update + jnp.dot(kept[source], block, preferred_element_type=jnp.float32)
                pair += 1
            residual = (sub_rhs[tree, level] - update).astype(jnp.bfloat16)
            inverse = diag_inverse[level, :, first_row:first_row + NS]
            solved = jnp.dot(residual, inverse, preferred_element_type=jnp.float32)
            levels_out.append(solved)
            kept.append(solved.astype(jnp.bfloat16))
        for source in range(LEVELS):
            factor = root_factor[source, first_row:first_row + NS]
            block = factor * expand(root_mask[source, first_tile:first_tile + TB])
            root_update = root_update + jnp.dot(kept[source], block, preferred_element_type=jnp.float32)
        results.append(jnp.stack(levels_out))
    root_residual = (root_rhs - root_update).astype(jnp.bfloat16)
    root_solution = jnp.dot(root_residual, root_inverse, preferred_element_type=jnp.float32)
    return jnp.concatenate(results, axis=2), root_solution
```

```python
import functools

import jax
import jax.numpy as jnp
from jax import lax
from jax.experimental import pallas as pl
from jax.experimental.pallas import tpu as pltpu
from jax.sharding import PartitionSpec as P

MESH = pl.DeviceIdType.MESH


def flip(index, distance):
    bit = 1
    while bit <= distance:
        if distance & bit:
            index = index + bit * (1 - 2 * lax.rem(lax.div(index, bit), 2))
        bit *= 2
    return index


def pair_of(level, source):
    return level * (level - 1) // 2 + source


def kernel(
    cfg,
    sub_rhs, root_rhs, diag_inverse, root_inverse, inner_factor, inner_mask, root_factor, root_mask,
    sub_out, root_out,
    rhs_v, root_rhs_v, diag_v, rinv_v, inner_v, root_v,
    part_p, recv_a, sum_a, recv_b, solved,
    part_r, recv_ra, sum_ra, recv_rb, solved_r,
    part_c, recv_rs, recv_x, full, early,
    load_sem, out_sem, send_p, recv_p, send_c, recv_c,
):
    levels, parts, owners, others, trees, bits, tile = (
        cfg["levels"], cfg["parts"], cfg["owners"], cfg["others"], cfg["trees"], cfg["bits"], cfg["tile"]
    )
    prow = lax.axis_index("prow")
    pcol = lax.axis_index("pcol")
    grid = lax.axis_index("grid")
    member = lax.rem(pcol, owners)
    tree = lax.div(pcol, owners)
    other = grid * trees + tree
    core = lax.rem(prow, 2)

    def prow_partner(bit):
        return {"prow": flip(prow, 1 << bit)}

    def pcol_partner(distance):
        return {"pcol": flip(pcol, distance)}

    def other_partner(distance):
        there = flip(other, distance)
        return {"grid": lax.div(there, trees), "pcol": lax.rem(there, trees) * owners + member}

    loads = {}

    def load(name, source, target):
        copy = pltpu.make_async_copy(source, target, load_sem.at[len(loads)])
        copy.start()
        loads[name] = copy

    load("rhs", sub_rhs.at[tree], rhs_v)
    load(("diag", 0), diag_inverse.at[0], diag_v.at[0])
    for level in range(1, levels):
        for source in range(level):
            if source == level - 1:
                load(("root", level - 1), root_factor.at[level - 1], root_v.at[level - 1])
            pair = pair_of(level, source)
            load(("inner", pair), inner_factor.at[pair], inner_v.at[pair])
        load(("diag", level), diag_inverse.at[level], diag_v.at[level])
    load(("root", levels - 1), root_factor.at[levels - 1], root_v.at[levels - 1])
    load("root_rhs", root_rhs, root_rhs_v)
    load("rinv", root_inverse, rinv_v)

    barrier = pltpu.get_barrier_semaphore()
    partners = [prow_partner(bit) for bit in range(bits)]
    partners += [pcol_partner(distance) for distance in range(1, owners)]
    partners += [other_partner(distance) for distance in range(1, others)]
    for partner in partners:
        pl.semaphore_signal(barrier, inc=1, device_id=partner, device_id_type=MESH)

    waited = set()

    def arrived(name):
        if name not in waited:
            waited.add(name)
            loads[name].wait()

    sends = []

    def send(source, target, send_sem, recv_sem, partner):
        copy = pltpu.make_async_remote_copy(
            src_ref=source, dst_ref=target, send_sem=send_sem, recv_sem=recv_sem,
            device_id=partner, device_id_type=MESH,
        )
        copy.start()
        sends.append(copy)
        return copy

    first_column = prow * (inner_v.shape[2] // tile)

    def mask_weights(kind, which):
        arrived((kind, which))
        weights, mask = (inner_v, inner_mask) if kind == "inner" else (root_v, root_mask)

        def mask_row(row, carry):
            rows = pl.ds(pl.multiple_of(row * tile, tile), tile)
            for column in range(weights.shape[2] // tile):
                columns = pl.ds(column * tile, tile)
                keep = mask[which, row, first_column + column].astype(jnp.float32)
                scale = jnp.full((tile, tile), keep, jnp.float32).astype(jnp.bfloat16)
                weights[which, rows, columns] = weights[which, rows, columns] * scale
            return carry

        lax.fori_loop(0, weights.shape[1] // tile, mask_row, 0)

    rows_of = [pl.ds(h * (rhs_v.shape[1] // parts), rhs_v.shape[1] // parts) for h in range(parts)]
    waits = {}
    outs = []

    def buffers(level):
        if level < levels:
            return [ref.at[level] for ref in (part_p, recv_a, sum_a, recv_b, solved)]
        return [part_r, recv_ra, sum_ra, recv_rb, solved_r]

    def solve(level, h):
        part, got, _, _, _ = buffers(level)
        if level < levels:
            arrived("rhs")
            residual = rhs_v[level, rows_of[h]]
        else:
            arrived("root_rhs")
            residual = root_rhs_v[rows_of[h]]
        if level > 0:
            for copy in waits.pop(("gather", level, h)):
                copy.wait_recv()
            update = full[level - 1, h]
            residual = residual - update.reshape(residual.shape)
        if level < levels:
            arrived(("diag", level))
            inverse = diag_v[level]
        else:
            arrived("rinv")
            inverse = rinv_v[...]
        product = jnp.dot(residual.astype(jnp.bfloat16), inverse, preferred_element_type=jnp.float32)
        part[h] = product.reshape(part.shape[1:])
        if level == 0 and h == 0:
            pl.semaphore_wait(barrier, len(partners))
        waits["a", level, h] = send(
            part.at[h, 1 - core], got.at[h], send_p.at[level, h, 0], recv_p.at[level, h, 0], prow_partner(0)
        )

    def chip_sum(level, h):
        part, got, total, far, _ = buffers(level)
        waits.pop(("a", level, h)).wait_recv()
        total[h, 0] = part[h, core] + got[h]
        waits["b", level, h] = send(
            total.at[h, 0], far.at[h, 0], send_p.at[level, h, 1], recv_p.at[level, h, 1], prow_partner(1)
        )

    def far_sum(level, h, bit):
        _, _, total, far, done = buffers(level)
        waits.pop(("b", level, h)).wait_recv()
        value = total[h, bit - 1] + far[h, bit - 1]
        if bit + 1 < bits:
            total[h, bit] = value
            waits["b", level, h] = send(
                total.at[h, bit], far.at[h, bit],
                send_p.at[level, h, bit + 1], recv_p.at[level, h, bit + 1], prow_partner(bit + 1),
            )
        else:
            done[h, core] = value
            waits["c", level, h] = send(
                done.at[h, core], done.at[h, core],
                send_p.at[level, h, bits], recv_p.at[level, h, bits], prow_partner(0),
            )

    def solution_here(level, h):
        done = buffers(level)[4]
        if ("c", level, h) in waits:
            waits.pop(("c", level, h)).wait_recv()
            for half in range(2):
                rows = done.shape[2]
                span = pl.ds(h * 2 * rows + half * rows, rows)
                target = sub_out.at[level, span] if level < levels else root_out.at[span]
                copy = pltpu.make_async_copy(done.at[h, half], target, out_sem.at[level, h, half])
                copy.start()
                outs.append(copy)

    def kept(level, h):
        value = solved[level, h]
        return value.reshape((-1, value.shape[-1])).astype(jnp.bfloat16)

    def weights_of(level, source):
        if level < levels:
            return inner_v[pair_of(level, source)]
        return root_v[source]

    def scatter(level, h):
        source = level - 1
        solution_here(source, h)
        product = jnp.dot(kept(source, h), weights_of(level, source), preferred_element_type=jnp.float32)
        if source > 0:
            product = product + early[level - 2, h]
        part_c[source, h] = product.reshape(part_c.shape[2:])
        copies = []
        for distance in range(owners - 1, 0, -1):
            copies.append(send(
                part_c.at[source, h, flip(member, distance)], recv_rs.at[source, h, distance],
                send_c.at[source, h, 0, distance], recv_c.at[source, h, 0, distance], pcol_partner(distance),
            ))
        waits["scatter", level, h] = copies

    def look_ahead(source, h):
        for level in range(source + 2, levels + 1):
            product = jnp.dot(kept(source, h), weights_of(level, source), preferred_element_type=jnp.float32)
            if source > 0:
                product = product + early[level - 2, h]
            early[level - 2, h] = product

    def gather(level, h, total):
        full[level - 1, h, member] = total
        copies = []
        for distance in range(owners - 1, 0, -1):
            copies.append(send(
                full.at[level - 1, h, member], full.at[level - 1, h, member],
                send_c.at[level - 1, h, 1, distance], recv_c.at[level - 1, h, 1, distance],
                pcol_partner(distance),
            ))
        waits["gather", level, h] = copies

    def reduce(level, h):
        total = part_c[level - 1, h, member]
        for copy, distance in zip(waits.pop(("scatter", level, h)), range(owners - 1, 0, -1)):
            copy.wait_recv()
            total = total + recv_rs[level - 1, h, distance]
        if level < levels or others == 1:
            gather(level, h, total)
            return
        recv_x[h, other] = total
        waits["others", level, h] = [
            send(
                recv_x.at[h, other], recv_x.at[h, other],
                send_c.at[level - 1, h, 2, distance], recv_c.at[level - 1, h, 2, distance],
                other_partner(distance),
            )
            for distance in range(1, others)
        ]

    def across(level, h):
        if ("others", level, h) not in waits:
            return
        for copy in waits.pop(("others", level, h)):
            copy.wait_recv()
        total = recv_x[h, 0]
        for index in range(1, others):
            total = total + recv_x[h, index]
        gather(level, h, total)

    def each(step, *args):
        for h in range(parts):
            step(args[0], h, *args[1:])

    for level in range(levels + 1):
        each(solve, level)
        if level == 0:
            mask_weights("inner", 0)
        each(chip_sum, level)
        if level < levels - 1:
            mask_weights("inner", level + 1)
        elif level < levels:
            mask_weights("root", level)
        for bit in range(1, bits):
            each(far_sum, level, bit)
        if level < levels:
            each(scatter, level + 1)
            if level + 1 < levels:
                mask_weights("root", level)
                each(look_ahead, level)
            each(reduce, level + 1)
            each(across, level + 1)
        else:
            each(solution_here, level)
    for copy in sends:
        copy.wait_send()
    for copy in outs:
        copy.wait()


def shards(sizes, *arrays):
    sub_rhs, root_rhs, diag_inverse, root_inverse, inner_factor, inner_mask, root_factor, root_mask = arrays
    levels, nrhs, here = sub_rhs.shape[1:]
    assert levels == 3 and sizes["prow"] >= 4
    columns = diag_inverse.shape[2]
    root_columns = root_inverse.shape[1]
    ns = here * sizes["prow"]
    owners = ns // columns
    trees = sizes["pcol"] // owners
    others = trees * sizes["grid"]
    bits = sizes["prow"].bit_length() - 1
    parts = 2 if nrhs // 2 // owners >= 8 else 1
    rows = nrhs // parts
    chunk = rows // owners
    cfg = dict(
        levels=levels, parts=parts, owners=owners, others=others, trees=trees, bits=bits,
        tile=inner_factor.shape[1] // inner_mask.shape[1],
    )
    f32 = jnp.float32

    def prow_buffers(lead, width):
        return [
            pltpu.VMEM((*lead, parts, 2, rows // 2, width), f32),
            pltpu.VMEM((*lead, parts, rows // 2, width), f32),
            pltpu.VMEM((*lead, parts, bits - 1, rows // 2, width), f32),
            pltpu.VMEM((*lead, parts, bits - 1, rows // 2, width), f32),
            pltpu.VMEM((*lead, parts, 2, rows // 2, width), f32),
        ]

    most = max(owners, others)
    dma = pltpu.SemaphoreType.DMA
    scratch = [
        pltpu.VMEM(sub_rhs.shape[1:], f32),
        pltpu.VMEM(root_rhs.shape, f32),
        pltpu.VMEM(diag_inverse.shape, jnp.bfloat16),
        pltpu.VMEM(root_inverse.shape, jnp.bfloat16),
        pltpu.VMEM(inner_factor.shape, jnp.bfloat16),
        pltpu.VMEM(root_factor.shape, jnp.bfloat16),
        *prow_buffers((levels,), columns),
        *prow_buffers((), root_columns),
        pltpu.VMEM((levels, parts, owners, chunk, here), f32),
        pltpu.VMEM((levels, parts, owners, chunk, here), f32),
        pltpu.VMEM((parts, others, chunk, here), f32),
        pltpu.VMEM((levels, parts, owners, chunk, here), f32),
        pltpu.VMEM((levels - 1, parts, rows, here), f32),
        dma((3 * levels + 3,)),
        dma((levels + 1, parts, 2)),
        dma((levels + 1, parts, bits + 1)),
        dma((levels + 1, parts, bits + 1)),
        dma((levels, parts, 3, most)),
        dma((levels, parts, 3, most)),
    ]
    anywhere = pl.BlockSpec(memory_space=pl.ANY)
    scalars = pl.BlockSpec(memory_space=pltpu.SMEM)
    return pl.pallas_call(
        functools.partial(kernel, cfg),
        out_shape=(
            jax.ShapeDtypeStruct((levels, nrhs, columns), f32),
            jax.ShapeDtypeStruct((nrhs, root_columns), f32),
        ),
        in_specs=[anywhere] * 5 + [scalars, anywhere, scalars],
        out_specs=(anywhere, anywhere),
        scratch_shapes=scratch,
        compiler_params=pltpu.CompilerParams(collective_id=0, has_side_effects=True),
    )(*arrays)


def solution(mesh):
    return jax.shard_map(
        functools.partial(shards, dict(mesh.shape)),
        mesh=mesh,
        in_specs=(
            P("grid", None, None, "prow"),
            P(None, "prow"),
            P(None, "prow", ("grid", "pcol")),
            P("prow", "grid"),
            P(None, ("grid", "pcol"), "prow"),
            P(None, ("grid", "pcol"), None),
            P(None, ("grid", "pcol"), "prow"),
            P(None, ("grid", "pcol"), None),
        ),
        out_specs=(P(None, None, ("grid", "pcol")), P(None, "grid")),
        check_vma=False,
    )
```

```python
import functools

import jax
import jax.numpy as jnp
from jax import lax
from jax.experimental import pallas as pl
from jax.experimental.pallas import tpu as pltpu
from jax.sharding import PartitionSpec as P

MESH = pl.DeviceIdType.MESH


def flip(index, distance):
    bit = 1
    while bit <= distance:
        if distance & bit:
            index = index + bit * (1 - 2 * lax.rem(lax.div(index, bit), 2))
        bit *= 2
    return index


def pair_of(level, source):
    return level * (level - 1) // 2 + source


def kernel(
    cfg,
    sub_rhs, root_rhs, diag_inverse, root_inverse, inner_factor, inner_mask, root_factor, root_mask,
    solved, solved_r,
    rhs_v, root_rhs_v, diag_v, rinv_v, inner_v, root_v,
    part_p, recv_a, sum_a, recv_b,
    part_r, recv_ra, sum_ra, recv_rb,
    part_c, recv_rs, recv_x, full, part_d, recv_d, full_d, early,
    load_sem, send_p, recv_p, send_c, recv_c,
):
    levels, parts, owners, others, trees, chips, tile, direct = (
        cfg["levels"], cfg["parts"], cfg["owners"], cfg["others"], cfg["trees"], cfg["chips"], cfg["tile"], cfg["direct"]
    )
    prow = lax.axis_index("prow")
    pcol = lax.axis_index("pcol")
    grid = lax.axis_index("grid")
    member = lax.rem(pcol, owners)
    tree = lax.div(pcol, owners)
    other = grid * trees + tree
    core = lax.rem(prow, 2)

    def prow_partner(distance):
        return {"prow": flip(prow, distance)}

    def pcol_partner(distance):
        return {"pcol": flip(pcol, distance)}

    def other_partner(distance, within=0):
        there = flip(other, distance)
        return {"grid": lax.div(there, trees), "pcol": lax.rem(there, trees) * owners + flip(member, within)}

    everyone = [(far, near) for far in range(others) for near in range(owners - 1, -1, -1) if far or near]

    loads = {}

    def load(name, source, target):
        copy = pltpu.make_async_copy(source, target, load_sem.at[len(loads)])
        copy.start()
        loads[name] = copy

    load(("rhs", 0), sub_rhs.at[tree, 0], rhs_v.at[0])
    load(("diag", 0), diag_inverse.at[0], diag_v.at[0])
    for level in range(1, levels):
        load(("rhs", level), sub_rhs.at[tree, level], rhs_v.at[level])
        for source in range(level):
            if source == level - 1:
                load(("root", level - 1), root_factor.at[level - 1], root_v.at[level - 1])
            pair = pair_of(level, source)
            load(("inner", pair), inner_factor.at[pair], inner_v.at[pair])
        load(("diag", level), diag_inverse.at[level], diag_v.at[level])
    load(("root", levels - 1), root_factor.at[levels - 1], root_v.at[levels - 1])
    load("root_rhs", root_rhs, root_rhs_v)
    load("rinv", root_inverse, rinv_v)

    barrier = pltpu.get_barrier_semaphore()
    partners = [prow_partner(distance) for distance in range(1, 2 * chips)]
    if direct:
        partners += [other_partner(far, near) for far, near in everyone]
    else:
        partners += [pcol_partner(distance) for distance in range(1, owners)]
        partners += [other_partner(distance) for distance in range(1, others)]
    for partner in partners:
        pl.semaphore_signal(barrier, inc=1, device_id=partner, device_id_type=MESH)

    waited = set()

    def arrived(name):
        if name not in waited:
            waited.add(name)
            loads[name].wait()

    sends = []

    def send(source, target, send_sem, recv_sem, partner):
        copy = pltpu.make_async_remote_copy(
            src_ref=source, dst_ref=target, send_sem=send_sem, recv_sem=recv_sem,
            device_id=partner, device_id_type=MESH,
        )
        copy.start()
        sends.append(copy)
        return copy

    first_column = prow * (inner_v.shape[2] // tile)

    def mask_weights(kind, which):
        arrived((kind, which))
        weights, mask = (inner_v, inner_mask) if kind == "inner" else (root_v, root_mask)

        def mask_row(row, carry):
            rows = pl.ds(pl.multiple_of(row * tile, tile), tile)
            for column in range(weights.shape[2] // tile):
                columns = pl.ds(column * tile, tile)
                keep = mask[which, row, first_column + column].astype(jnp.float32)
                scale = jnp.full((tile, tile), keep, jnp.float32).astype(jnp.bfloat16)
                weights[which, rows, columns] = weights[which, rows, columns] * scale
            return carry

        lax.fori_loop(0, weights.shape[1] // tile, mask_row, 0)

    rows_of = [pl.ds(h * (rhs_v.shape[1] // parts), rhs_v.shape[1] // parts) for h in range(parts)]
    waits = {}

    def buffers(level):
        if level < levels:
            return [ref.at[level] for ref in (part_p, recv_a, sum_a, recv_b, solved)]
        return [part_r, recv_ra, sum_ra, recv_rb, solved_r]

    def solve(level, h):
        part, got, _, _, _ = buffers(level)
        if level < levels:
            arrived(("rhs", level))
            residual = rhs_v[level, rows_of[h]]
        else:
            arrived("root_rhs")
            residual = root_rhs_v[rows_of[h]]
        if level > 0:
            for copy in waits.pop(("gather", level, h)):
                copy.wait_recv()
            if level == levels and direct:
                update = jnp.concatenate([full_d[h, far].reshape((residual.shape[0], -1)) for far in range(others)], axis=1)
            else:
                update = full[level - 1, h].reshape(residual.shape)
            residual = residual - update
        if level < levels:
            arrived(("diag", level))
            inverse = diag_v[level]
        else:
            arrived("rinv")
            inverse = rinv_v[...]
        product = jnp.dot(residual.astype(jnp.bfloat16), inverse, preferred_element_type=jnp.float32)
        part[h] = product.reshape(part.shape[1:])
        if level == 0 and h == 0:
            pl.semaphore_wait(barrier, len(partners))
        waits["a", level, h] = send(
            part.at[h], got.at[h], send_p.at[level, h, 0], recv_p.at[level, h, 0], prow_partner(1)
        )

    def chip_sum(level, h):
        part, got, total, far, _ = buffers(level)
        waits.pop(("a", level, h)).wait_recv()
        total[h, core] = part[h, core] + got[h, core]
        waits["b", level, h] = [
            send(
                total.at[h, core], far.at[h, distance - 2],
                send_p.at[level, h, distance], recv_p.at[level, h, distance], prow_partner(distance),
            )
            for distance in range(2, 2 * chips)
        ]
        total[h, 1 - core] = part[h, 1 - core] + got[h, 1 - core]

    def far_sum(level, h):
        _, _, total, far, done = buffers(level)
        copies = waits.pop(("b", level, h))
        for cross in range(2):
            half = core if cross == 0 else 1 - core
            value = total[h, half]
            for slot in range(cross, len(copies), 2):
                copies[slot].wait_recv()
                value = value + far[h, slot]
            done[h, half] = value

    def kept(level, h):
        value = solved[level, h]
        return value.reshape((-1, value.shape[-1])).astype(jnp.bfloat16)

    def weights_of(level, source):
        if level < levels:
            return inner_v[pair_of(level, source)]
        return root_v[source]

    def scatter(level, h):
        source = level - 1
        product = jnp.dot(kept(source, h), weights_of(level, source), preferred_element_type=jnp.float32)
        if source > 0:
            product = product + early[level - 2, h]
        if level == levels and direct:
            width = part_d.shape[-1]
            for far in range(others):
                part_d[h, far] = product[:, far * width:(far + 1) * width].reshape(part_d.shape[2:])
            waits["scatter", level, h] = [
                send(
                    part_d.at[h, flip(other, far), flip(member, near)], recv_d.at[h, far, near],
                    send_c.at[source, h, 2 * far, near], recv_c.at[source, h, 2 * far, near],
                    other_partner(far, near),
                )
                for far, near in everyone
            ]
            return
        part_c[source, h] = product.reshape(part_c.shape[2:])
        copies = []
        for distance in range(owners - 1, 0, -1):
            copies.append(send(
                part_c.at[source, h, flip(member, distance)], recv_rs.at[source, h, distance],
                send_c.at[source, h, 0, distance], recv_c.at[source, h, 0, distance], pcol_partner(distance),
            ))
        waits["scatter", level, h] = copies

    def look_ahead(source, h):
        for level in range(source + 2, levels + 1):
            product = jnp.dot(kept(source, h), weights_of(level, source), preferred_element_type=jnp.float32)
            if source > 0:
                product = product + early[level - 2, h]
            early[level - 2, h] = product

    def gather(level, h, total):
        full[level - 1, h, member] = total
        copies = []
        for distance in range(owners - 1, 0, -1):
            copies.append(send(
                full.at[level - 1, h, member], full.at[level - 1, h, member],
                send_c.at[level - 1, h, 1, distance], recv_c.at[level - 1, h, 1, distance],
                pcol_partner(distance),
            ))
        waits["gather", level, h] = copies

    def reduce(level, h):
        if level == levels and direct:
            total = part_d[h, other, member]
            for copy, (far, near) in zip(waits.pop(("scatter", level, h)), everyone):
                copy.wait_recv()
                total = total + recv_d[h, far, near]
            full_d[h, other, member] = total
            waits["gather", level, h] = [
                send(
                    full_d.at[h, other, member], full_d.at[h, other, member],
                    send_c.at[level - 1, h, 2 * far + 1, near], recv_c.at[level - 1, h, 2 * far + 1, near],
                    other_partner(far, near),
                )
                for far, near in everyone
            ]
            return
        total = part_c[level - 1, h, member]
        for copy, distance in zip(waits.pop(("scatter", level, h)), range(owners - 1, 0, -1)):
            copy.wait_recv()
            total = total + recv_rs[level - 1, h, distance]
        if level < levels or others == 1:
            gather(level, h, total)
            return
        recv_x[h, other] = total
        waits["others", level, h] = [
            send(
                recv_x.at[h, other], recv_x.at[h, other],
                send_c.at[level - 1, h, 2, distance], recv_c.at[level - 1, h, 2, distance],
                other_partner(distance),
            )
            for distance in range(1, others)
        ]

    def across(level, h):
        if ("others", level, h) not in waits:
            return
        for copy in waits.pop(("others", level, h)):
            copy.wait_recv()
        total = recv_x[h, 0]
        for index in range(1, others):
            total = total + recv_x[h, index]
        gather(level, h, total)

    def each(step, *args):
        for h in range(parts):
            step(args[0], h, *args[1:])

    for level in range(levels + 1):
        each(solve, level)
        if level == 0:
            mask_weights("inner", 0)
        each(chip_sum, level)
        if level < levels - 1:
            mask_weights("inner", level + 1)
        elif level < levels:
            mask_weights("root", level)
        each(far_sum, level)
        if level < levels:
            each(scatter, level + 1)
            if level + 1 < levels:
                mask_weights("root", level)
                each(look_ahead, level)
            each(reduce, level + 1)
            each(across, level + 1)
    for copy in sends:
        copy.wait_send()


def shards(sizes, *arrays):
    sub_rhs, root_rhs, diag_inverse, root_inverse, inner_factor, inner_mask, root_factor, root_mask = arrays
    levels, nrhs, here = sub_rhs.shape[1:]
    assert levels == 3 and sizes["prow"] >= 4
    columns = diag_inverse.shape[2]
    root_columns = root_inverse.shape[1]
    ns = here * sizes["prow"]
    owners = ns // columns
    trees = sizes["pcol"] // owners
    others = trees * sizes["grid"]
    chips = sizes["prow"] // 2
    parts = 2 if nrhs // 2 // owners >= 8 else 1
    rows = nrhs // parts
    chunk = rows // owners
    direct = others > 1 and here % (others * 128) == 0
    width = here // others if direct else 128
    cfg = dict(
        levels=levels, parts=parts, owners=owners, others=others, trees=trees, chips=chips,
        tile=inner_factor.shape[1] // inner_mask.shape[1], direct=direct,
    )
    f32 = jnp.float32

    def prow_buffers(lead, width):
        half = (rows // 2, width)
        return [
            pltpu.VMEM((*lead, parts, 2, *half), f32),
            pltpu.VMEM((*lead, parts, 2, *half), f32),
            pltpu.VMEM((*lead, parts, 2, *half), f32),
            pltpu.VMEM((*lead, parts, 2 * chips - 2, *half), f32),
        ]

    most = max(owners, others)
    dma = pltpu.SemaphoreType.DMA
    scratch = [
        pltpu.VMEM(sub_rhs.shape[1:], f32),
        pltpu.VMEM(root_rhs.shape, f32),
        pltpu.VMEM(diag_inverse.shape, jnp.bfloat16),
        pltpu.VMEM(root_inverse.shape, jnp.bfloat16),
        pltpu.VMEM(inner_factor.shape, jnp.bfloat16),
        pltpu.VMEM(root_factor.shape, jnp.bfloat16),
        *prow_buffers((levels,), columns),
        *prow_buffers((), root_columns),
        pltpu.VMEM((levels, parts, owners, chunk, here), f32),
        pltpu.VMEM((levels, parts, owners, chunk, here), f32),
        pltpu.VMEM((parts, others, chunk, here), f32),
        pltpu.VMEM((levels, parts, owners, chunk, here), f32),
        pltpu.VMEM((parts, others, owners, chunk, width), f32),
        pltpu.VMEM((parts, others, owners, chunk, width), f32),
        pltpu.VMEM((parts, others, owners, chunk, width), f32),
        pltpu.VMEM((levels - 1, parts, rows, here), f32),
        dma((levels * (levels - 1) // 2 + 3 * levels + 2,)),
        dma((levels + 1, parts, 2 * chips)),
        dma((levels + 1, parts, 2 * chips)),
        dma((levels, parts, max(3, 2 * others), most)),
        dma((levels, parts, max(3, 2 * others), most)),
    ]
    anywhere = pl.BlockSpec(memory_space=pl.ANY)
    scalars = pl.BlockSpec(memory_space=pltpu.SMEM)
    sub_out, root_out = pl.pallas_call(
        functools.partial(kernel, cfg),
        out_shape=(
            pltpu.VMEM((levels, parts, 2, rows // 2, columns), f32),
            pltpu.VMEM((parts, 2, rows // 2, root_columns), f32),
        ),
        in_specs=[anywhere] * 5 + [scalars, anywhere, scalars],
        out_specs=(pl.BlockSpec(memory_space=pltpu.VMEM), pl.BlockSpec(memory_space=pltpu.VMEM)),
        scratch_shapes=scratch,
        compiler_params=pltpu.CompilerParams(collective_id=0, has_side_effects=True),
    )(*arrays)
    return sub_out.reshape((levels, nrhs, columns)), root_out.reshape((nrhs, root_columns))


def solution(mesh):
    return jax.shard_map(
        functools.partial(shards, dict(mesh.shape)),
        mesh=mesh,
        in_specs=(
            P("grid", None, None, "prow"),
            P(None, "prow"),
            P(None, "prow", ("grid", "pcol")),
            P("prow", "grid"),
            P(None, ("grid", "pcol"), "prow"),
            P(None, ("grid", "pcol"), None),
            P(None, ("grid", "pcol"), "prow"),
            P(None, ("grid", "pcol"), None),
        ),
        out_specs=(P(None, None, ("grid", "pcol")), P(None, "grid")),
        check_vma=False,
    )
```
